256 devices in a mesh: rows: 64 (over y, z, core), vocab: 4 (over x).
Axes of the slice: x: 4, y: 4, z: 8, core: 2. Of those that a mesh axis runs over, the one named last changes fastest.
Arguments:
- hidden_policy: bfloat16 [4096, 1536], P('rows', 'vocab'), may hold values from -45 to 45
- hidden_reference: bfloat16 [4096, 1536], P('rows', 'vocab'), may hold values from -45 to 45
- gain_policy: bfloat16 [1536], replicated, may hold values from 0.5 to 1.5
- gain_reference: bfloat16 [1536], replicated, may hold values from 0.5 to 1.5
- head_policy: bfloat16 [1536, 131072], P(None, ('rows', 'vocab')), may hold values from -20 to 20
- head_reference: bfloat16 [1536, 131072], P(None, ('rows', 'vocab')), may hold values from -20 to 20
- targets: int32 [4096], P('rows'), may hold values from 0 to 131071
- loss_mask: int32 [4096], P('rows'), may hold values from 0 to 1, as said below
- doc_lengths: int32 [128], replicated, may hold values from 1 to 127, as said below
- doc_owner: int32 [128], replicated, may hold values from 0 to 63, as said below
- doc_score: float32 [128], replicated, may hold values from -3 to 6
Outputs:
- token_logprob: float32 [8192], P('rows')
- doc_advantage: float32 [128], P('rows')
The draws below stay inside these ranges and needn't reach their ends.
Inputs may be any that keep to these rules, and one draw needn't show every extreme that they name: `loss_mask`: each index of rows holds at most 32 ones among its 64 tokens, and some index holds exactly 32. `doc_lengths`: documents lie end to end in the pack in this order; their lengths add up to 4096. `doc_owner`: every index of rows owns exactly 2 documents, whose lengths add up to at most 128; for some index they add up to exactly 128.
All inputs are finite; a program needn't handle non-finite values.
Results may differ from the reference program's by a relative error of at most 0.0025.
Values may be sent and summed in bfloat16 or wider, within the bound.
No kernel may reach another device: no remote copies, remote signals or barrier semaphores. Data moves between devices by JAX's collectives and lax.ppermute only.
A program may use at most 128 MiB of HBM per device.

```python
import math
import jax
import jax.numpy as jnp
from jax import lax

D = 1536
VOC_DEV = 512
TOK_DEV = 64
DOC_DEV = 2
TOKENS = 4096
VOCAB = 131072
RESP_DEV = 32
CAP = 128
DOCS = 128
N_ROWS = 64


anchor_count = 4


anchor_strengths = (1.0, 1.7, 2.4, 3.0)


anchor_logit = 110.0


anchor_gap = 1.9


def doc_layout(key):
    stream = jax.random.fold_in(key, 11)
    key_one, key_two, key_three, key_four = jax.random.split(stream, 4)
    pairing = jax.random.permutation(key_one, N_ROWS)
    pair_count = N_ROWS // 2
    swing = jax.random.randint(key_two, (pair_count,), 0, TOK_DEV - DOC_DEV + 1)
    swing_one = swing[1] % (TOK_DEV - 2 * DOC_DEV + 1)
    larger = (TOK_DEV + swing).at[0].set(2 * TOK_DEV).at[1].set(TOK_DEV + swing_one)
    smaller = (TOK_DEV - swing).at[0].set(DOC_DEV).at[1].set(TOK_DEV - DOC_DEV - swing_one)
    totals = jnp.zeros((N_ROWS,), jnp.int32).at[pairing[0::2]].set(larger.astype(jnp.int32)).at[pairing[1::2]].set(smaller.astype(jnp.int32))
    weights = jax.random.randint(key_three, (N_ROWS, DOC_DEV), 1, 64)
    single_row = (jnp.arange(DOC_DEV, dtype=jnp.int32) == 0).astype(weights.dtype)
    weights = weights.at[pairing[0]].set(single_row)
    running = jnp.cumsum(weights, axis=1)
    cut_points = (totals[:, None] - DOC_DEV) * running // running[:, -1:]
    previous = jnp.concatenate([jnp.zeros((N_ROWS, 1), jnp.int32), cut_points[:, :-1].astype(jnp.int32)], axis=1)
    doc_lens = (1 + cut_points - previous).reshape(-1).astype(jnp.int32)
    owners = jnp.repeat(jnp.arange(N_ROWS, dtype=jnp.int32), DOC_DEV)
    shuffle = jax.random.permutation(key_four, DOCS)
    return (doc_lens[shuffle], owners[shuffle])


def anchor_set(key):
    anchors = jnp.clip(jax.random.normal(jax.random.fold_in(key, 90), (anchor_count, D), jnp.float32), -3.0, 3.0)
    positions = jax.random.permutation(jax.random.fold_in(key, 91), TOKENS)[:anchor_count]
    columns = jax.random.permutation(jax.random.fold_in(key, 92), VOCAB)[:2 * anchor_count]
    return (anchors, positions, columns)


def hidden_common(key, which):
    stream = jax.random.fold_in(key, 40 + which)
    key_one, key_two, key_three = jax.random.split(stream, 3)
    row_scale = jnp.exp(jax.random.uniform(key_two, (TOKENS, 1), jnp.float32, math.log(0.3), math.log(3.0)))
    col_scale = jnp.exp(jax.random.uniform(key_three, (1, D), jnp.float32, math.log(0.3), math.log(3.0)))
    values = jnp.clip(jax.random.normal(key_one, (TOKENS, D), jnp.float32), -4.0, 4.0) * row_scale * col_scale
    anchors, positions, columns = anchor_set(key)
    values = values.at[positions].set(anchors)
    return values.astype(jnp.bfloat16)


def head_common(key, which):
    stream = jax.random.fold_in(key, 60 + which)
    spread = 3.0 / math.sqrt(D)
    values = jnp.clip(jax.random.normal(stream, (D, VOCAB), jnp.float32), -4.0, 4.0) * spread
    anchors, positions, columns = anchor_set(key)
    strengths = jnp.array(anchor_strengths, jnp.float32)
    strong = anchors.T * strengths[None, :] * (anchor_logit / D)
    nearby = anchors.T * (strengths[None, :] - anchor_gap / anchor_logit) * (anchor_logit / D)
    values = values.at[:, columns[:anchor_count]].set(strong + 0.1 * values[:, columns[:anchor_count]])
    values = values.at[:, columns[anchor_count:]].set(nearby + 0.1 * values[:, columns[anchor_count:]])
    return values.astype(jnp.bfloat16)


def draw_hidden_policy(key, part):
    return hidden_common(key, 1)


def draw_hidden_reference(key, part):
    return hidden_common(key, 2)


def draw_head_policy(key, part):
    return head_common(key, 1)


def draw_head_reference(key, part):
    return head_common(key, 2)


def draw_loss_mask(key, part):
    stream = jax.random.fold_in(key, 21)
    key_one, key_two, key_three = jax.random.split(stream, 3)
    counts = jax.random.randint(key_one, (N_ROWS,), RESP_DEV - RESP_DEV // 2, RESP_DEV + 1)
    forced = jax.random.randint(key_two, (), 0, N_ROWS)
    counts = counts.at[forced].set(RESP_DEV)
    shuffled = jax.vmap(lambda subkey: jax.random.permutation(subkey, TOK_DEV))(jax.random.split(key_three, N_ROWS))
    return (shuffled < counts[:, None]).astype(jnp.int32).reshape(-1)


def draw_doc_lengths(key, part):
    doc_lens, owners = doc_layout(key)
    return doc_lens


def draw_doc_owner(key, part):
    doc_lens, owners = doc_layout(key)
    return owners


def draw_doc_score(key, part):
    doc_lens, owners = doc_layout(key)
    growth = 1.0 + 2.0 * owners.astype(jnp.float32) / (N_ROWS - 1)
    stream = jax.random.fold_in(key, 30)
    uniform_part = jax.random.uniform(stream, (DOCS,), jnp.float32, 0.5, 1.5)
    return uniform_part * growth


def with_ends(drawn, own_key, smallest, high):
    index_at = [jax.random.randint(jax.random.fold_in(own_key, axis), (), 0, length) for axis, length in enumerate(drawn.shape)]
    longest = drawn.shape.index(max(drawn.shape))
    next_to = index_at[:longest] + [(index_at[longest] + 1) % drawn.shape[longest]] + index_at[longest + 1:]
    return drawn.at[tuple(index_at)].set(smallest).at[tuple(next_to)].set(high)


def setup_inputs(seed: int = 0) -> dict:
    key_of = jax.random.split(jax.random.key(seed), 12)
    hidden_policy = draw_hidden_policy(jax.random.fold_in(key_of[11], 71), 0)
    hidden_reference = draw_hidden_reference(jax.random.fold_in(key_of[11], 71), 0)
    gain_policy = jnp.clip(1.0 + 0.1 * jax.random.normal(key_of[2], (D,), jnp.float32), 0.5, 1.5).astype(jnp.bfloat16)
    gain_reference = jnp.clip(1.0 + 0.1 * jax.random.normal(key_of[3], (D,), jnp.float32), 0.5, 1.5).astype(jnp.bfloat16)
    head_policy = draw_head_policy(jax.random.fold_in(key_of[11], 71), 0)
    head_reference = draw_head_reference(jax.random.fold_in(key_of[11], 71), 0)
    targets = with_ends(jax.random.randint(key_of[6], (TOKENS,), 0, VOCAB), jax.random.fold_in(key_of[6], 1), 0, VOCAB - 1).astype(jnp.int32)
    loss_mask = draw_loss_mask(jax.random.fold_in(key_of[11], 71), 0)
    doc_lengths = draw_doc_lengths(jax.random.fold_in(key_of[11], 71), 0)
    doc_owner = draw_doc_owner(jax.random.fold_in(key_of[11], 71), 0)
    doc_score = draw_doc_score(jax.random.fold_in(key_of[11], 71), 0)
    return {"hidden_policy": hidden_policy, "hidden_reference": hidden_reference, "gain_policy": gain_policy, "gain_reference": gain_reference, "head_policy": head_policy, "head_reference": head_reference, "targets": targets, "loss_mask": loss_mask, "doc_lengths": doc_lengths, "doc_owner": doc_owner, "doc_score": doc_score}


epsilon = 1e-06
kl_weight = 0.1

def final_norm(hidden, gain_vector):
    values = hidden.astype(jnp.float32)
    inverse_rms = lax.rsqrt(lax.optimization_barrier(jnp.mean(values * values, axis=1, keepdims=True)) + epsilon)
    return (values * inverse_rms * gain_vector.astype(jnp.float32)[None, :]).astype(jnp.bfloat16)

def token_logprobs(normed, head, targets):
    block_width = VOC_DEV * 8
    row_count = normed.shape[0]

    def advance(running, block_index):
        highest, exp_total = running
        head_block = lax.dynamic_slice_in_dim(head, block_index * block_width, block_width, 1)
        logits = jnp.dot(normed, head_block, preferred_element_type=jnp.float32)
        new_highest = jnp.maximum(highest, lax.optimization_barrier(jnp.max(logits, axis=1)))
        exp_total = exp_total * jnp.exp(highest - new_highest) + lax.optimization_barrier(jnp.sum(jnp.exp(logits - new_highest[:, None]), axis=1))
        return ((new_highest, exp_total), None)
    initial = (jnp.full((row_count,), -jnp.inf, jnp.float32), jnp.zeros((row_count,), jnp.float32))
    blocks = jnp.arange(head.shape[1] // block_width, dtype=jnp.int32)
    (highest, exp_total), _ = lax.scan(advance, initial, blocks)
    picked = jnp.take(head, targets, axis=1).astype(jnp.float32)
    target_logit = lax.optimization_barrier(jnp.sum(normed.astype(jnp.float32) * picked.T, axis=1))
    return target_logit - (highest + jnp.log(exp_total))

def doc_tables(doc_lengths, doc_owner):
    starts = (jnp.cumsum(doc_lengths) - doc_lengths).astype(jnp.int32)
    doc_order = jnp.arange(doc_lengths.shape[0], dtype=jnp.int32)
    before = ((doc_owner[None, :] == doc_owner[:, None]) & (doc_order[None, :] < doc_order[:, None])).astype(jnp.int32)
    offset = lax.optimization_barrier(jnp.sum(before * doc_lengths[None, :], axis=1)).astype(jnp.int32)
    doc_rank = lax.optimization_barrier(jnp.sum(before, axis=1)).astype(jnp.int32)
    return (starts, offset, doc_rank)

def slot_table(owner_index, starts, offset, doc_rank, doc_lengths, doc_owner, slot_count):
    slot_index = jnp.arange(slot_count, dtype=jnp.int32)[:, None]
    inside = ((doc_owner[None, :] == owner_index) & (slot_index >= offset[None, :]) & (slot_index < offset[None, :] + doc_lengths[None, :])).astype(jnp.int32)
    slot_token = lax.optimization_barrier(jnp.sum(inside * (starts[None, :] + slot_index - offset[None, :]), axis=1)).astype(jnp.int32)
    slot_filled = lax.optimization_barrier(jnp.sum(inside, axis=1)).astype(jnp.int32)
    slot_doc = lax.optimization_barrier(jnp.sum(inside * doc_rank[None, :], axis=1)).astype(jnp.int32)
    return (slot_token, slot_filled, slot_doc)

def document_rewards(policy_lp, reference_lp, slot_mask, slot_doc, owner_index, doc_owner, doc_rank, doc_score, doc_slots):
    weights_mask = slot_mask.astype(jnp.float32)
    log_ratio = policy_lp - reference_lp
    kl_term = 0.5 * log_ratio * log_ratio
    doc_number = jnp.arange(doc_slots, dtype=jnp.int32)[:, None]
    doc_pick = (slot_doc[None, :] == doc_number).astype(jnp.float32)
    counts = lax.optimization_barrier(jnp.sum(doc_pick * weights_mask[None, :], axis=1))
    kl_sum = lax.optimization_barrier(jnp.sum(doc_pick * (weights_mask * kl_term)[None, :], axis=1))
    chosen = ((doc_owner[None, :] == owner_index) & (doc_rank[None, :] == doc_number)).astype(jnp.float32)
    doc_value = lax.optimization_barrier(jnp.sum(chosen * doc_score[None, :], axis=1))
    reward = doc_value - kl_weight * kl_sum / jnp.maximum(counts, 1.0)
    return (reward, counts)

def reference(hidden_policy, hidden_reference, gain_policy, gain_reference, head_policy, head_reference, targets, loss_mask, doc_lengths, doc_owner, doc_score):
    normed_policy = final_norm(hidden_policy, gain_policy)
    normed_reference = final_norm(hidden_reference, gain_reference)
    logprob_policy = token_logprobs(normed_policy, head_policy, targets)
    logprob_reference = token_logprobs(normed_reference, head_reference, targets)
    starts, offset, doc_rank = doc_tables(doc_lengths, doc_owner)

    def per_owner(owner_index):
        slot_token, slot_filled, slot_doc = slot_table(owner_index, starts, offset, doc_rank, doc_lengths, doc_owner, CAP)
        slot_mask = jnp.take(loss_mask, slot_token) * slot_filled
        policy_lp = jnp.take(logprob_policy, slot_token)
        reference_lp = jnp.take(logprob_reference, slot_token)
        token_logprob = jnp.where(slot_mask == 1, policy_lp, 0.0)
        reward, counts = document_rewards(policy_lp, reference_lp, slot_mask, slot_doc, owner_index, doc_owner, doc_rank, doc_score, DOC_DEV)
        return (token_logprob, reward, counts)
    token_logprob, reward, counts = jax.vmap(per_owner)(jnp.arange(N_ROWS, dtype=jnp.int32))
    baseline = jnp.sum(counts * reward) / jnp.sum(counts)
    return (token_logprob.reshape(-1), (reward - baseline).reshape(-1))
```

```python
import functools

import jax
import jax.numpy as jnp
from jax import lax
from jax.experimental import pallas as pl
from jax.experimental.pallas import tpu as pltpu
from jax.sharding import Mesh
from jax.sharding import PartitionSpec as P

DOC_DEV = 2
CAP = 128
LANES = 128
ROWS = ("y", "z", "c")
X = ("xh", "xl")
ALL = ("y", "z", "c", "xh", "xl")

epsilon = 1e-06
kl_weight = 0.1
f32 = jnp.float32
bf16 = jnp.bfloat16
VMEM = pl.BlockSpec(memory_space=pltpu.VMEM)
SMEM = pl.BlockSpec(memory_space=pltpu.SMEM)
ANY = pl.BlockSpec(memory_space=pl.ANY)


def iota(shape, dim):
    return lax.broadcasted_iota(jnp.int32, shape, dim)


def as_column(row):
    n = row.shape[1]
    return jnp.sum(jnp.where(iota((n, n), 0) == iota((n, n), 1), row, 0), axis=1, keepdims=True)


def pick_kernel(where_ref, hp_ref, hr_ref, tgt_ref, mask_ref, out_ref, ids_ref):
    tok = hp_ref.shape[0]
    kept = tok // 2
    nz, nx, tiles, half, _ = out_ref.shape
    per = (tiles - 1) // 2
    mask_row = mask_ref[...]
    mask_col = as_column(mask_row)
    sub, lane = iota((tok, tok), 0), iota((tok, tok), 1)
    rank_row = jnp.sum(jnp.where(sub <= lane, mask_col, 0), axis=0, keepdims=True) - 1
    rank_col = jnp.sum(jnp.where(lane <= sub, mask_row, 0), axis=1, keepdims=True) - 1
    select = (iota((kept, tok), 0) == rank_row) & (mask_row == 1)
    one_hot = select.astype(f32).astype(bf16)
    target = jnp.sum(jnp.where(select, tgt_ref[...], 0), axis=1, keepdims=True)
    spot = iota((kept, LANES), 1)
    digit = jnp.where(
        spot == 0,
        target & 63,
        jnp.where(spot == 1, (target >> 6) & 63, jnp.where(spot == 2, target >> 12, 0)),
    )
    digit = digit.astype(f32).astype(bf16)
    packed = [
        jnp.dot(one_hot, ref[...], preferred_element_type=f32).astype(bf16)
        for ref in (hp_ref, hr_ref)
    ]
    for h in range(2):
        lines = slice(h * half, (h + 1) * half)
        pieces = [
            packed[m][lines, j * LANES : (j + 1) * LANES] for m in range(2) for j in range(per)
        ] + [digit[lines]]
        for z in range(nz):
            for x in range(h, nx, 2):
                for t, piece in enumerate(pieces):
                    out_ref[z, x, t] = piece
    first, base = where_ref[0], where_ref[1]
    wanted = iota((tok, LANES), 1)
    found = (rank_col == wanted + first) & (mask_col == 1) & (wanted < 8)
    place = jnp.sum(jnp.where(found, iota((tok, LANES), 0) + base + 1, 0), axis=0, keepdims=True)
    ids_ref[...] = (place - 1).astype(f32)


def norm_kernel(in_ref, gain_ref, out_ref):
    nz, nx, tiles, half, _ = in_ref.shape
    per = (tiles - 1) // 2
    width = nx * per * LANES
    for z in range(nz):
        for m in range(2):
            parts = [
                in_ref[z, x, m * per + j].astype(f32) for x in range(nx) for j in range(per)
            ]
            square = parts[0] * parts[0]
            for part in parts[1:]:
                square = square + part * part
            mean = jnp.sum(square, axis=1, keepdims=True) * (1.0 / width)
            inverse = lax.rsqrt(mean + epsilon)
            for k, part in enumerate(parts):
                gain = gain_ref[m, :, k * LANES : (k + 1) * LANES].astype(f32)
                out_ref[z, m * nx * per + k] = (part * inverse * gain).astype(bf16)
        out_ref[z, 2 * nx * per] = in_ref[z, 0, tiles - 1]


def logits_kernel(base_ref, *refs):
    ny = len(refs) - 8 - 5
    toks, heads = refs[:ny], refs[ny : ny + 8]
    out_ref, lhs, held, logit, sem = refs[ny + 8 :]
    copies = [pltpu.make_async_copy(heads[i], held.at[i], sem.at[i]) for i in range(8)]
    for copy in copies:
        copy.start()
    nz, tiles, half, _ = toks[0].shape
    per = (tiles - 1) // 2
    total = ny * nz * half
    for y in range(ny):
        for z in range(nz):
            line = (y * nz + z) * half
            for m in range(2):
                for k in range(per):
                    lhs[m, line : line + half, k * LANES : (k + 1) * LANES] = toks[y][z, m * per + k]
    digit = jnp.concatenate(
        [toks[y][:, tiles - 1].reshape(nz * half, LANES) for y in range(ny)], axis=0
    ).astype(f32)
    target = (digit[:, 0:1] + 64.0 * digit[:, 1:2] + 4096.0 * digit[:, 2:3]).astype(jnp.int32)
    columns = held.shape[2]

    def one_shard(i, state):
        high, summed, hit = state
        for k in range(8):

            @pl.when(i == k)
            def _():
                copies[k].wait()

        logit[...] = jnp.dot(lhs[i // 4], held[i], preferred_element_type=f32)
        values = logit[...]
        here = jnp.max(values, axis=1, keepdims=True)
        fresh = lax.rem(i, 4) == 0
        old_high = jnp.where(fresh, here, high)
        new_high = jnp.maximum(old_high, here)
        part = jnp.sum(jnp.exp(values - new_high), axis=1, keepdims=True)
        summed = jnp.where(fresh, 0.0, summed) * jnp.exp(old_high - new_high) + part
        match = iota((total, columns), 1) == target - base_ref[i]
        hit = jnp.where(fresh, 0.0, hit) + jnp.sum(
            jnp.where(match, values, 0.0), axis=1, keepdims=True
        )
        return new_high, summed, hit

    zero = jnp.zeros((total, 1), f32)
    policy = lax.fori_loop(0, 4, one_shard, (zero, zero, zero))
    other = lax.fori_loop(4, 8, one_shard, (zero, zero, zero))
    lane, line = iota((total, LANES), 1), iota((total, LANES), 0)
    spot = lane - (line & 7)
    wide = jnp.zeros((total, LANES), f32)
    for k, (high, summed, hit) in enumerate((policy, other)):
        wide = jnp.where(spot == 16 * k, high + jnp.log(summed), wide)
        wide = jnp.where(spot == 16 * k + 8, hit, wide)
    out_ref[:, 0, :] = jnp.sum(wide.reshape(total // 8, 8, LANES), axis=1)


def merge_kernel(in_ref, ids_ref, out_ref):
    values = in_ref[:, 0, :]
    high = jnp.max(values, axis=0, keepdims=True)
    lse = high + jnp.log(jnp.sum(jnp.exp(values - high), axis=0, keepdims=True))
    hit = jnp.sum(values, axis=0, keepdims=True)
    logprob = hit - pltpu.roll(jnp.broadcast_to(lse, (8, LANES)), 8, 1)
    ratio = logprob - pltpu.roll(logprob, LANES - 16, 1)
    kl = pltpu.roll(0.5 * ratio * ratio, 8, 1)
    lane = iota((8, LANES), 1)
    line = jnp.where(
        lane < 8, ids_ref[...], jnp.where(lane < 16, logprob, jnp.where(lane < 24, kl, 0.0))
    )
    out_ref[...] = jnp.broadcast_to(line[0:1][:, None, :], out_ref.shape)


def docs_kernel(me_ref, in_ref, len_ref, owner_ref, score_ref, token_ref, doc_ref):
    me = me_ref[0]
    length, owner, score = len_ref[...], owner_ref[...], score_ref[...]
    n = length.shape[1]
    sub, lane = iota((n, n), 0), iota((n, n), 1)
    length_col, owner_col = as_column(length), as_column(owner)
    earlier = sub < lane
    start = jnp.sum(jnp.where(earlier, length_col, 0), axis=0, keepdims=True)
    before = earlier & (owner_col == owner)
    offset = jnp.sum(jnp.where(before, length_col, 0), axis=0, keepdims=True)
    rank = jnp.sum(jnp.where(before, 1, 0), axis=0, keepdims=True)
    start_col, offset_col = as_column(start), as_column(offset)
    inside = (owner_col == me) & (lane >= offset_col) & (lane < offset_col + length_col)
    slot = jnp.sum(jnp.where(inside, start_col + lane - offset_col + 1, 0), axis=0, keepdims=True)
    slot_id = jnp.where(slot > 0, slot - 1, -7).astype(f32)
    low, high = start.astype(f32), (start + length).astype(f32)
    table = in_ref[:, 0, :]
    count = jnp.zeros((table.shape[0], n), f32)
    kl_sum, logprob = count, count
    for j in range(8):
        place = table[:, j : j + 1]
        within = (place >= low) & (place < high)
        count = count + jnp.where(within, 1.0, 0.0)
        kl_sum = kl_sum + jnp.where(within, table[:, 16 + j : 17 + j], 0.0)
        logprob = logprob + jnp.where(place == slot_id, table[:, 8 + j : 9 + j], 0.0)
    count = jnp.sum(count, axis=0, keepdims=True)
    kl_sum = jnp.sum(kl_sum, axis=0, keepdims=True)
    token_ref[...] = jnp.sum(logprob, axis=0, keepdims=True)
    reward = score - kl_weight * kl_sum / jnp.maximum(count, 1.0)
    baseline = jnp.sum(count * reward, axis=1, keepdims=True) / jnp.sum(
        count, axis=1, keepdims=True
    )
    advantage = jnp.broadcast_to(reward - baseline, (8, n))
    first = jnp.sum(
        jnp.where((owner == me) & (rank == 0), advantage, 0.0), axis=1, keepdims=True
    )
    second = jnp.sum(
        jnp.where((owner == me) & (rank == 1), advantage, 0.0), axis=1, keepdims=True
    )
    spot = iota((8, n), 1)
    doc_ref[...] = jnp.where(spot == 0, first, jnp.where(spot == 1, second, 0.0))[0:1]


def shape_of(shape, dtype):
    return jax.ShapeDtypeStruct(shape, dtype)


def shifted(x, axis, by):
    n = lax.axis_size(axis)
    return lax.ppermute(x, axis, [(i, (i + by) % n) for i in range(n)])


def per_device(
    hidden_policy,
    hidden_reference,
    gain_policy,
    gain_reference,
    head_policy,
    head_reference,
    targets,
    loss_mask,
    doc_lengths,
    doc_owner,
    doc_score,
):
    ny, nz, nx = lax.axis_size("y"), lax.axis_size("z"), lax.axis_size(X)
    tok, width = hidden_policy.shape
    columns = head_policy.shape[1]
    per, half = width // LANES, tok // 4
    me, x = lax.axis_index(ROWS), lax.axis_index(X)
    xh, xl, c = lax.axis_index("xh"), lax.axis_index("xl"), lax.axis_index("c")

    pair_policy = [(i, i ^ 1) for i in range(nx)]
    pair_reference = [(i, (i + 1) % nx if i % 2 else (i - 1) % nx) for i in range(nx)]
    near_policy = lax.ppermute(head_policy, X, pair_policy)
    near_reference = lax.ppermute(head_reference, X, pair_reference)
    heads = [
        head_policy,
        shifted(head_policy, "c", 1),
        near_policy,
        shifted(near_policy, "c", 1),
        head_reference,
        shifted(head_reference, "c", 1),
        near_reference,
        shifted(near_reference, "c", 1),
    ]
    x_policy = x ^ 1
    x_reference = jnp.where(x % 2 == 1, (x + 1) % nx, (x + nx - 1) % nx)
    row_of = me - c
    bases = jnp.stack(
        [
            ((row_of + core) * nx + place) * columns
            for partner in (x_policy, x_reference)
            for place in (x, partner)
            for core in (c, 1 - c)
        ]
    ).astype(jnp.int32)

    tiles = 2 * per + 1
    where = jnp.stack([xl * half + xh * 8, me * tok]).astype(jnp.int32)
    sent, ids = pl.pallas_call(
        pick_kernel,
        out_shape=(
            shape_of((nz, nx, tiles, half, LANES), bf16),
            shape_of((1, LANES), f32),
        ),
        in_specs=[SMEM, VMEM, VMEM, VMEM, VMEM],
        out_specs=(VMEM, VMEM),
        name="pick",
    )(where, hidden_policy, hidden_reference, targets[None, :], loss_mask[None, :])
    got = lax.all_to_all(
        sent.reshape(nz * nx, tiles, half, LANES), ("z", *X), 0, 0, tiled=True
    ).reshape(nz, nx, tiles, half, LANES)
    wide = 2 * nx * per + 1
    gains = jnp.stack([gain_policy, gain_reference])[:, None, :]
    normed = pl.pallas_call(
        norm_kernel,
        out_shape=shape_of((nz, wide, half, LANES), bf16),
        in_specs=[VMEM, VMEM],
        out_specs=VMEM,
        name="norm",
    )(got, gains)
    full = lax.all_to_all(
        jnp.broadcast_to(normed[None], (ny, *normed.shape)), "y", 0, 0, tiled=True
    )
    total = ny * nz * half
    stats = pl.pallas_call(
        logits_kernel,
        out_shape=shape_of((total // 8, 1, LANES), f32),
        in_specs=[SMEM] + [VMEM] * ny + [ANY] * 8,
        out_specs=VMEM,
        scratch_shapes=[
            pltpu.VMEM((2, total, nx * width), bf16),
            pltpu.VMEM((8, nx * width, columns), bf16),
            pltpu.VMEM((total, columns), f32),
            pltpu.SemaphoreType.DMA((8,)),
        ],
        compiler_params=pltpu.CompilerParams(vmem_limit_bytes=48 * 1024 * 1024),
        cost_estimate=pl.CostEstimate(
            flops=2 * 8 * total * nx * width * columns, bytes_accessed=1 << 24, transcendentals=0
        ),
        name="logits",
    )(bases, *[full[k] for k in range(ny)], *heads)
    merged = lax.all_to_all(stats, ("y", "z", "xh"), 0, 0, tiled=True)
    line = pl.pallas_call(
        merge_kernel,
        out_shape=shape_of((lax.axis_size(ALL), 1, LANES), f32),
        in_specs=[VMEM, VMEM],
        out_specs=VMEM,
        name="merge",
    )(merged, ids)
    table = lax.all_to_all(line, ALL, 0, 0, tiled=True)
    token_logprob, advantage = pl.pallas_call(
        docs_kernel,
        out_shape=(shape_of((1, CAP), f32), shape_of((1, CAP), f32)),
        in_specs=[SMEM] + [VMEM] * 4,
        out_specs=(VMEM, VMEM),
        name="docs",
    )(
        jnp.stack([me]).astype(jnp.int32),
        table,
        doc_lengths[None, :],
        doc_owner[None, :],
        doc_score[None, :],
    )
    return token_logprob.reshape(CAP), advantage[0, :DOC_DEV]


def solution(mesh):
    finer = Mesh(
        mesh.devices.reshape(4, 8, 2, 2, mesh.shape["vocab"] // 2), ("y", "z", "c", "xh", "xl")
    )
    placed = (
        P(ROWS, X),
        P(ROWS, X),
        P(),
        P(),
        P(None, ALL),
        P(None, ALL),
        P(ROWS),
        P(ROWS),
        P(),
        P(),
        P(),
    )
    return jax.shard_map(
        per_device, mesh=finer, in_specs=placed, out_specs=(P(ROWS), P(ROWS)), check_vma=False
    )
```

```python
import functools

import jax
import jax.numpy as jnp
from jax import lax
from jax.experimental import pallas as pl
from jax.experimental.pallas import tpu as pltpu
from jax.sharding import Mesh
from jax.sharding import PartitionSpec as P


DOC_DEV = 2
CAP = 128
LANES = 128
ROWS = ("y", "z", "c")
X = ("xh", "xl")
ALL = ("y", "z", "c", "xh", "xl")

epsilon = 1e-06
kl_weight = 0.1
f32 = jnp.float32
bf16 = jnp.bfloat16
VMEM = pl.BlockSpec(memory_space=pltpu.VMEM)
SMEM = pl.BlockSpec(memory_space=pltpu.SMEM)
ANY = pl.BlockSpec(memory_space=pl.ANY)


def iota(shape, dim):
    return lax.broadcasted_iota(jnp.int32, shape, dim)


def as_column(row):
    n = row.shape[1]
    return jnp.sum(jnp.where(iota((n, n), 0) == iota((n, n), 1), row, 0), axis=1, keepdims=True)


def pick_kernel(hp_ref, hr_ref, tgt_ref, mask_ref, out_ref):
    tok = hp_ref.shape[0]
    kept, half = tok // 2, tok // 4
    nz, nx, lines, _ = out_ref.shape
    per = (lines - 8) // half // 2
    mask_row = mask_ref[...]
    mask_col = as_column(mask_row)
    sub, lane = iota((tok, tok), 0), iota((tok, tok), 1)
    rank = jnp.sum(jnp.where(sub <= lane, mask_col, 0), axis=0, keepdims=True) - 1
    select = (iota((kept, tok), 0) == rank) & (mask_row == 1)
    one_hot = select.astype(f32).astype(bf16)
    target = jnp.sum(jnp.where(select, tgt_ref[...], 0), axis=1, keepdims=True)
    place = jnp.sum(
        jnp.where(select, iota((kept, tok), 1) + 1, 0), axis=1, keepdims=True
    )
    packed = [
        jnp.dot(one_hot, ref[...], preferred_element_type=f32).astype(bf16)
        for ref in (hp_ref, hr_ref)
    ]
    spot = iota((8, LANES), 1)
    for h in range(2):
        digits = jnp.zeros((8, LANES), jnp.int32)
        for g in range(2):
            part = slice(h * half + g * 8, h * half + g * 8 + 8)
            for k, value in enumerate(
                (target[part] & 63, (target[part] >> 6) & 63, target[part] >> 12, place[part])
            ):
                digits = jnp.where(spot == 4 * g + k, value, digits)
        digits = digits.astype(f32).astype(bf16)
        rows = slice(h * half, (h + 1) * half)
        pieces = [
            packed[m][rows, j * LANES : (j + 1) * LANES] for m in range(2) for j in range(per)
        ]
        for z in range(nz):
            for x in range(h, nx, 2):
                for t, piece in enumerate(pieces):
                    out_ref[z, x, t * half : (t + 1) * half] = piece
                out_ref[z, x, 2 * per * half :] = digits


def norm_kernel(in_ref, gp_ref, gr_ref, *out_refs):
    nz, nx, lines, _ = in_ref.shape
    half = 16
    per = (lines - 8) // half // 2
    width = nx * per * LANES
    share = nz // len(out_refs)
    for z in range(nz):
        out_ref, at = out_refs[z // share], z % share
        for m, gain_ref in enumerate((gp_ref, gr_ref)):
            parts = [
                in_ref[z, x, (m * per + j) * half : (m * per + j + 1) * half].astype(f32)
                for x in range(nx)
                for j in range(per)
            ]
            square = parts[0] * parts[0]
            for part in parts[1:]:
                square = square + part * part
            mean = jnp.sum(square, axis=1, keepdims=True) * (1.0 / width)
            inverse = lax.rsqrt(mean + epsilon)
            for k, part in enumerate(parts):
                gain = gain_ref[:, k * LANES : (k + 1) * LANES].astype(f32)
                t = m * nx * per + k
                out_ref[at, t * half : (t + 1) * half] = (part * inverse * gain).astype(bf16)
        out_ref[at, 2 * nx * per * half :] = in_ref[z, 0, 2 * per * half :]


def logits_kernel(base_ref, where_ref, *refs):
    toks, heads = refs[:8], refs[8:16]
    out_ref, lhs, held, even, odd, sem = refs[16:]
    copies = [pltpu.make_async_copy(heads[i], held.at[i], sem.at[i]) for i in range(8)]
    for copy in copies:
        copy.start()
    half = 16
    share, lines, _ = toks[0].shape
    per = (lines - 8) // half // 2
    nz = 2 * share
    ny = len(toks) // 2
    total = ny * nz * half
    columns = held.shape[2]
    target, place = [], []
    for y in range(ny):
        for z in range(nz):
            tok = toks[2 * y + z // share]
            at = z % share
            line = (y * nz + z) * half
            for m in range(2):
                for k in range(per):
                    t = m * per + k
                    lhs[m, line : line + half, k * LANES : (k + 1) * LANES] = tok[
                        at, t * half : (t + 1) * half
                    ]
            digit = tok[at, 2 * per * half :].astype(f32)
            for g in (0, 4):
                target.append(
                    digit[:, g : g + 1]
                    + 64.0 * digit[:, g + 1 : g + 2]
                    + 4096.0 * digit[:, g + 2 : g + 3]
                )
                place.append(digit[:, g + 3 : g + 4])
    target = jnp.concatenate(target, axis=0).astype(jnp.int32)
    place = jnp.concatenate(place, axis=0)
    column = iota((total, columns), 1)

    def product(i, out):
        for k in range(8):

            @pl.when(i == k)
            def _():
                copies[k].wait()

        out[...] = jnp.dot(lhs[i // 4], held[i], preferred_element_type=f32)

    def reduce(i, out, state):
        high, summed, hit = state
        values = out[...]
        fresh = lax.rem(i, 4) == 0
        here = jnp.max(values, axis=1, keepdims=True)
        old_high = jnp.where(fresh, here, high)
        new_high = jnp.maximum(old_high, here)
        part = jnp.sum(jnp.exp(values - new_high), axis=1, keepdims=True)
        summed = jnp.where(fresh, 0.0, summed) * jnp.exp(old_high - new_high) + part
        match = column == target - base_ref[i]
        hit = jnp.where(fresh, 0.0, hit) + jnp.sum(
            jnp.where(match, values, 0.0), axis=1, keepdims=True
        )
        return new_high, summed, hit

    def two(j, state):
        product(2 * j + 1, odd)
        state = reduce(2 * j, even, state)
        product(2 * j + 2, even)
        return reduce(2 * j + 1, odd, state)

    zero = jnp.zeros((total, 1), f32)
    product(0, even)
    policy = lax.fori_loop(0, 2, two, (zero, zero, zero))
    other = two(2, policy)
    product(7, odd)
    other = reduce(7, odd, reduce(6, even, other))
    row = nz * half
    diagonal = iota((row, LANES), 0) == iota((row, LANES), 1)
    for y in range(ny):
        to = where_ref[y]
        at = slice(y * row, (y + 1) * row)
        for v, value in enumerate(
            (
                policy[0] + jnp.log(policy[1]),
                policy[2],
                other[0] + jnp.log(other[1]),
                other[2],
                place,
            )
        ):
            line = jnp.sum(jnp.where(diagonal, value[at], 0.0), axis=0, keepdims=True)
            if v == 4:
                z = iota((1, LANES), 1) // half
                line = jnp.where(line > 0.0, line + (where_ref[4 + y] + 128 * z).astype(f32), 0.0)
            out_ref[pl.ds(4 * v + to, 1)] = line
    out_ref[20:24] = jnp.zeros((4, LANES), f32)


def total_of(lines):
    out = lines[0]
    for line in lines[1:]:
        out = out + line
    return out


def lse_of(lines):
    high = functools.reduce(jnp.maximum, lines)
    return high + jnp.log(total_of([jnp.exp(line - high) for line in lines]))


def merge_kernel(in_ref, out_ref):
    sources = in_ref.shape[0]
    for c in range(2):
        lines = [in_ref[s] for s in range(c, sources, 2)]
        lse, added = lse_of(lines), total_of(lines)
        for v in range(5):
            part = slice(4 * v, 4 * v + 4)
            value = (lse, added, lse, added, lines[0])[v]
            for k in range(out_ref.shape[0]):
                out_ref[k, v, 4 * c : 4 * c + 4] = value[part]


def as_row(column):
    n = column.shape[0]
    return jnp.sum(jnp.where(iota((n, n), 0) == iota((n, n), 1), column, 0), axis=0, keepdims=True)


def tables_kernel(me_ref, len_ref, owner_ref, score_ref, out_ref):
    me = me_ref[0]
    length, owner = len_ref[...], owner_ref[...]
    n = length.shape[1]
    sub, lane = iota((n, n), 0), iota((n, n), 1)
    length_col, owner_col = as_column(length), as_column(owner)
    earlier = lane < sub
    start = jnp.sum(jnp.where(earlier, length, 0), axis=1, keepdims=True)
    before = earlier & (owner_col == owner)
    offset = jnp.sum(jnp.where(before, length, 0), axis=1, keepdims=True)
    rank = jnp.sum(jnp.where(before, 1, 0), axis=1, keepdims=True)
    inside = (owner_col == me) & (lane >= offset) & (lane < offset + length_col)
    slot = jnp.sum(jnp.where(inside, start + lane - offset + 1, 0), axis=0, keepdims=True)
    slot = jnp.where(slot > 0, slot, -7)
    mine = owner_col == me
    table = jnp.zeros((n, n), f32)
    for k, value in enumerate(
        (
            start + 1,
            start + length_col + 1,
            as_column(slot),
            jnp.where(mine & (rank == 0), 1, 0),
            jnp.where(mine & (rank == 1), 1, 0),
        )
    ):
        table = jnp.where(lane == k, value.astype(f32), table)
    out_ref[...] = jnp.where(lane == 5, as_column(score_ref[...]), table)


def docs_kernel(in_ref, table_ref, token_ref, doc_ref):
    sources = in_ref.shape[0]
    table = table_ref[...]
    n = table.shape[0]
    low, high, slot, first, second, score = (table[:, k : k + 1] for k in range(6))
    count = jnp.zeros((n, LANES), f32)
    kl_sum, logprob = count, count
    for xl in range(2):
        lines = [[in_ref[s, v] for s in range(xl, sources, 2)] for v in range(5)]
        policy = total_of(lines[1]) - lse_of(lines[0])
        ratio = policy - (total_of(lines[3]) - lse_of(lines[2]))
        kl = 0.5 * ratio * ratio
        place = lines[4][0]
        for r in range(8):
            at = place[r : r + 1]
            within = (at >= low) & (at < high)
            count = count + jnp.where(within, 1.0, 0.0)
            kl_sum = kl_sum + jnp.where(within, kl[r : r + 1], 0.0)
            logprob = logprob + jnp.where(at == slot, policy[r : r + 1], 0.0)
    count = jnp.sum(count, axis=1, keepdims=True)
    kl_sum = jnp.sum(kl_sum, axis=1, keepdims=True)
    token_ref[...] = as_row(jnp.sum(logprob, axis=1, keepdims=True))
    reward = score - kl_weight * kl_sum / jnp.maximum(count, 1.0)
    baseline = jnp.sum(count * reward, axis=0, keepdims=True) / jnp.sum(
        count, axis=0, keepdims=True
    )
    advantage = reward - baseline
    doc_ref[:, 0:1] = jnp.sum(first * advantage, axis=0, keepdims=True)
    doc_ref[:, 1:2] = jnp.sum(second * advantage, axis=0, keepdims=True)


def shape_of(shape, dtype):
    return jax.ShapeDtypeStruct(shape, dtype)


def shifted(x, axis, by):
    n = lax.axis_size(axis)
    return lax.ppermute(x, axis, [(i, (i + by) % n) for i in range(n)])


def one_device(
    hidden_policy,
    hidden_reference,
    gain_policy,
    gain_reference,
    head_policy,
    head_reference,
    targets,
    loss_mask,
    doc_lengths,
    doc_owner,
    doc_score,
):
    ny, nz, nx = lax.axis_size("y"), lax.axis_size("z"), lax.axis_size(X)
    tok, width = hidden_policy.shape
    columns = head_policy.shape[1]
    per, half = width // LANES, tok // 4
    me, x = lax.axis_index(ROWS), lax.axis_index(X)
    c = lax.axis_index("c")

    pair_policy = [(i, i ^ 1) for i in range(nx)]
    pair_reference = [(i, (i + 1) % nx if i % 2 else (i - 1) % nx) for i in range(nx)]
    near_policy = lax.ppermute(head_policy, X, pair_policy)
    near_reference = lax.ppermute(head_reference, X, pair_reference)
    swapped = [shifted(near_policy, "c", 1), shifted(near_reference, "c", 1)]
    heads = [
        head_policy,
        shifted(head_policy, "c", 1),
        near_policy,
        swapped[0],
        head_reference,
        shifted(head_reference, "c", 1),
        near_reference,
        swapped[1],
    ]
    x_policy = x ^ 1
    x_reference = jnp.where(x % 2 == 1, (x + 1) % nx, (x + nx - 1) % nx)
    row_of = me - c
    bases = jnp.stack(
        [
            ((row_of + core) * nx + place) * columns
            for partner in (x_policy, x_reference)
            for place in (x, partner)
            for core in (c, 1 - c)
        ]
    ).astype(jnp.int32)

    lines = 2 * per * half + 8
    sent = pl.pallas_call(
        pick_kernel,
        out_shape=shape_of((nz, nx, lines, LANES), bf16),
        in_specs=[VMEM] * 4,
        out_specs=VMEM,
        name="pick",
    )(hidden_policy, hidden_reference, targets[None, :], loss_mask[None, :])
    got = lax.all_to_all(
        sent.reshape(nz * nx, lines, LANES), ("z", *X), 0, 0, tiled=True
    ).reshape(nz, nx, lines, LANES)
    wide = 2 * nx * per * half + 8
    own = pl.pallas_call(
        norm_kernel,
        out_shape=[shape_of((nz // 2, wide, LANES), bf16)] * 2,
        in_specs=[VMEM] * 3,
        out_specs=[VMEM] * 2,
        name="norm",
    )(got, gain_policy[None, :], gain_reference[None, :])
    below = [shifted(part, "y", 1) for part in own]
    above = [shifted(part, "y", -1) for part in own]
    far = [shifted(below[0], "y", 1), shifted(above[1], "y", -1)]
    lengths, _ = lax.optimization_barrier((doc_lengths, (below, above)))
    table = pl.pallas_call(
        tables_kernel,
        out_shape=shape_of((LANES, LANES), f32),
        in_specs=[SMEM] + [VMEM] * 3,
        out_specs=VMEM,
        name="tables",
    )(
        jnp.stack([me]).astype(jnp.int32),
        lengths[None, :],
        doc_owner[None, :],
        doc_score[None, :],
    )
    y = lax.axis_index("y")
    order = [y, (y + ny - 1) % ny, (y + 1) % ny, (y + 2) % ny]
    where = jnp.stack(order + [(row * nz * 2 + c) * tok for row in order]).astype(jnp.int32)
    total = ny * nz * half
    stats = pl.pallas_call(
        logits_kernel,
        out_shape=shape_of((24, LANES), f32),
        in_specs=[SMEM] * 2 + [VMEM] * 8 + [ANY] * 8,
        out_specs=VMEM,
        scratch_shapes=[
            pltpu.VMEM((2, total, nx * width), bf16),
            pltpu.VMEM((8, nx * width, columns), bf16),
            pltpu.VMEM((total, columns), f32),
            pltpu.VMEM((total, columns), f32),
            pltpu.SemaphoreType.DMA((8,)),
        ],
        compiler_params=pltpu.CompilerParams(vmem_limit_bytes=48 * 1024 * 1024),
        cost_estimate=pl.CostEstimate(
            flops=2 * 8 * total * nx * width * columns, bytes_accessed=1 << 24, transcendentals=0
        ),
        name="logits",
    )(bases, where, *own, *below, *above, *far, *heads)
    group = 2 * nz
    gathered = lax.all_to_all(
        jnp.broadcast_to(stats[None], (group, *stats.shape)), ("z", "c"), 0, 0, tiled=True
    )
    group = ny * nx
    merged = pl.pallas_call(
        merge_kernel,
        out_shape=shape_of((group, 5, 8, LANES), f32),
        in_specs=[VMEM],
        out_specs=VMEM,
        name="merge",
    )(gathered)
    everything = lax.all_to_all(merged, ("y", *X), 0, 0, tiled=True)
    token_logprob, advantage = pl.pallas_call(
        docs_kernel,
        out_shape=(shape_of((1, CAP), f32), shape_of((1, DOC_DEV), f32)),
        in_specs=[VMEM] * 2,
        out_specs=(VMEM, VMEM),
        name="docs",
    )(everything, table)
    return token_logprob.reshape(CAP), advantage.reshape(DOC_DEV)


def solution(mesh):
    finer = Mesh(
        mesh.devices.reshape(4, 8, 2, 2, mesh.shape["vocab"] // 2), ("y", "z", "c", "xh", "xl")
    )
    placed = (
        P(ROWS, X),
        P(ROWS, X),
        P(),
        P(),
        P(None, ALL),
        P(None, ALL),
        P(ROWS),
        P(ROWS),
        P(),
        P(),
        P(),
    )
    return jax.shard_map(
        one_device, mesh=finer, in_specs=placed, out_specs=(P(ROWS), P(ROWS)), check_vma=False
    )
```

```python
import functools

import jax
import jax.numpy as jnp
from jax import lax
from jax.experimental import pallas as pl
from jax.experimental.pallas import tpu as pltpu
from jax.sharding import Mesh
from jax.sharding import PartitionSpec as P


DOC_DEV = 2
CAP = 128
LANES = 128
ROWS = ("y", "z", "c")
X = ("xh", "xl")
ALL = ("y", "z", "c", "xh", "xl")

epsilon = 1e-06
kl_weight = 0.1
f32 = jnp.float32
bf16 = jnp.bfloat16
VMEM = pl.BlockSpec(memory_space=pltpu.VMEM)
SMEM = pl.BlockSpec(memory_space=pltpu.SMEM)
ANY = pl.BlockSpec(memory_space=pl.ANY)


def iota(shape, dim):
    return lax.broadcasted_iota(jnp.int32, shape, dim)


def as_column(row):
    n = row.shape[1]
    return jnp.sum(jnp.where(iota((n, n), 0) == iota((n, n), 1), row, 0), axis=1, keepdims=True)


def pick_kernel(hp_ref, hr_ref, tgt_ref, mask_ref, out_ref):
    tok = hp_ref.shape[0]
    kept, half = tok // 2, tok // 4
    nz, nx, lines, _ = out_ref.shape
    per = (lines - 8) // half // 2
    mask_row = mask_ref[...]
    mask_col = as_column(mask_row)
    sub, lane = iota((tok, tok), 0), iota((tok, tok), 1)
    rank = jnp.sum(jnp.where(sub <= lane, mask_col, 0), axis=0, keepdims=True) - 1
    select = (iota((kept, tok), 0) == rank) & (mask_row == 1)
    one_hot = select.astype(f32).astype(bf16)
    target = jnp.sum(jnp.where(select, tgt_ref[...], 0), axis=1, keepdims=True)
    place = jnp.sum(
        jnp.where(select, iota((kept, tok), 1) + 1, 0), axis=1, keepdims=True
    )
    packed = [
        jnp.dot(one_hot, ref[...], preferred_element_type=f32).astype(bf16)
        for ref in (hp_ref, hr_ref)
    ]
    spot = iota((8, LANES), 1)
    for h in range(2):
        digits = jnp.zeros((8, LANES), jnp.int32)
        for g in range(2):
            part = slice(h * half + g * 8, h * half + g * 8 + 8)
            for k, value in enumerate(
                (target[part] & 63, (target[part] >> 6) & 63, target[part] >> 12, place[part])
            ):
                digits = jnp.where(spot == 4 * g + k, value, digits)
        digits = digits.astype(f32).astype(bf16)
        rows = slice(h * half, (h + 1) * half)
        pieces = [
            packed[m][rows, j * LANES : (j + 1) * LANES] for m in range(2) for j in range(per)
        ]
        for z in range(nz):
            for x in range(h, nx, 2):
                for t, piece in enumerate(pieces):
                    out_ref[z, x, t * half : (t + 1) * half] = piece
                out_ref[z, x, 2 * per * half :] = digits


def norm_kernel(in_ref, gp_ref, gr_ref, *out_refs):
    nz, nx, lines, _ = in_ref.shape
    half = 16
    per = (lines - 8) // half // 2
    width = nx * per * LANES
    share = nz // len(out_refs)
    for z in range(nz):
        out_ref, at = out_refs[z // share], z % share
        for m, gain_ref in enumerate((gp_ref, gr_ref)):
            parts = [
                in_ref[z, x, (m * per + j) * half : (m * per + j + 1) * half].astype(f32)
                for x in range(nx)
                for j in range(per)
            ]
            square = parts[0] * parts[0]
            for part in parts[1:]:
                square = square + part * part
            mean = jnp.sum(square, axis=1, keepdims=True) * (1.0 / width)
            inverse = lax.rsqrt(mean + epsilon)
            for k, part in enumerate(parts):
                gain = gain_ref[:, k * LANES : (k + 1) * LANES].astype(f32)
                t = m * nx * per + k
                out_ref[at, t * half : (t + 1) * half] = (part * inverse * gain).astype(bf16)
        out_ref[at, 2 * nx * per * half :] = in_ref[z, 0, 2 * per * half :]


def place_lines(tok, lhs, line):
    half = 16
    share, lines, _ = tok.shape
    per = (lines - 8) // half // 2
    for at in range(share):
        for m in range(2):
            for k in range(per):
                t = m * per + k
                lhs[m, line : line + half, k * LANES : (k + 1) * LANES] = tok[
                    at, t * half : (t + 1) * half
                ]
        line += half


def columns_of(digit_refs):
    target, place = [], []
    for ref in digit_refs:
        for at in range(ref.shape[0]):
            digit = ref[at].astype(f32)
            for g in (0, 4):
                target.append(
                    digit[:, g : g + 1]
                    + 64.0 * digit[:, g + 1 : g + 2]
                    + 4096.0 * digit[:, g + 2 : g + 3]
                )
                place.append(digit[:, g + 3 : g + 4])
    return jnp.concatenate(target, axis=0).astype(jnp.int32), jnp.concatenate(place, axis=0)


def scores(lhs, rows, target, shards, heads, base_ref, buffers, waits):
    total, columns = rows.stop - rows.start, heads.shape[2]
    column = iota((total, columns), 1)

    def product(i, out):
        if i in waits:
            waits.pop(i).wait()
        out[0:total] = jnp.dot(lhs[i // 4, rows], heads[i], preferred_element_type=f32)

    def reduce(i, out, state):
        values = out[0:total]
        new_high = jnp.max(values, axis=1, keepdims=True)
        match = column == target - base_ref[i]
        new_hit = jnp.sum(jnp.where(match, values, 0.0), axis=1, keepdims=True)
        if state is None:
            part = jnp.sum(jnp.exp(values - new_high), axis=1, keepdims=True)
            return new_high, part, new_hit
        high, summed, hit = state
        new_high = jnp.maximum(high, new_high)
        part = jnp.sum(jnp.exp(values - new_high), axis=1, keepdims=True)
        return new_high, summed * jnp.exp(high - new_high) + part, hit + new_hit

    found = [None, None]
    product(shards[0], buffers[0])
    for n, i in enumerate(shards):
        if n + 1 < len(shards):
            product(shards[n + 1], buffers[(n + 1) % 2])
        found[i // 4] = reduce(i, buffers[n % 2], found[i // 4])
    return [
        value for high, summed, hit in found for value in (high + jnp.log(summed), hit)
    ]


def as_line(column):
    diagonal = iota((LANES, LANES), 0) == iota((LANES, LANES), 1)
    return jnp.sum(jnp.where(diagonal, column, 0.0), axis=0, keepdims=True)


def bring(sources, into, sem):
    copies = [pltpu.make_async_copy(ref, into.at[k], sem.at[k]) for k, ref in enumerate(sources)]
    for copy in copies:
        copy.start()
    return copies


def local_kernel(blocks, base_ref, *refs):
    sources, head_sources = refs[: 2 * blocks], refs[2 * blocks : 2 * blocks + 4]
    out_ref, lhs, toks, even, odd, heads, tok_sem, sem = refs[2 * blocks + 4 :]
    shards = (0, 1, 4, 5)
    arriving = bring(sources, toks, tok_sem)
    waits = {
        i: pltpu.make_async_copy(source, heads.at[i], sem.at[n])
        for n, (i, source) in enumerate(zip(shards, head_sources))
    }
    for copy in waits.values():
        copy.start()
    for k, copy in enumerate(arriving):
        copy.wait()
        place_lines(toks.at[k], lhs, k * LANES // 2)
    last = toks.shape[2] - 8
    target, _ = columns_of([toks.at[k, :, last:] for k in range(2 * blocks)])
    rows = slice(0, blocks * LANES)
    values = scores(lhs, rows, target, shards, heads, base_ref, (even, odd), waits)
    for b in range(blocks):
        for v, value in enumerate(values):
            out_ref[b, v : v + 1] = as_line(value[b * LANES : (b + 1) * LANES])
        out_ref[b, 4:8] = jnp.zeros((4, LANES), f32)


def far_kernel(base_ref, where_ref, *refs):
    sources, head_sources, done, packed = refs[:8], refs[8:16], refs[16:18], refs[18:20]
    out_ref, toks, digits, lhs, even, odd, heads, tok_sem, digit_sem, pack_sem, sem = refs[20:]
    lines = sources[0].shape[1]
    arriving = bring(sources[6:], toks, tok_sem)
    arriving += bring([ref.at[:, lines - 8 :] for ref in sources], digits, digit_sem)
    for k, (start, stop) in enumerate(((0, LANES), (LANES, 3 * LANES))):
        copy = pltpu.make_async_copy(packed[k], lhs.at[:, start:stop], pack_sem.at[k])
        copy.start()
        arriving.append(copy)
    order = (2, 3, 6, 7, 0, 1, 4, 5)
    waits = {i: pltpu.make_async_copy(head_sources[i], heads.at[i], sem.at[i]) for i in order}
    for copy in waits.values():
        copy.start()
    for copy in arriving:
        copy.wait()
    near = 3 * LANES
    place_lines(toks.at[0], lhs, near)
    place_lines(toks.at[1], lhs, near + LANES // 2)
    target, place = columns_of([digits.at[k] for k in range(8)])
    first = scores(
        lhs, slice(0, near), target[:near], (2, 3, 6, 7), heads, base_ref, (even, odd), waits
    )
    last = scores(
        lhs,
        slice(near, near + LANES),
        target[near:],
        (2, 3, 0, 1, 6, 7, 4, 5),
        heads,
        base_ref,
        (even, odd),
        waits,
    )
    index_z = iota((1, LANES), 1) // 16
    for b in range(4):
        at = slice(b * LANES, (b + 1) * LANES)
        for v in range(5):
            if v == 4:
                line = as_line(place[at])
                line = jnp.where(
                    line > 0.0, line + (where_ref[4 + b] + 128 * index_z).astype(f32), 0.0
                )
            elif b == 3:
                line = as_line(last[v])
            else:
                local = done[0][0, v : v + 1] if b == 0 else done[1][b - 1, v : v + 1]
                line = as_line(first[v][at])
                line = lse_of([line, local]) if v % 2 == 0 else line + local
            for k in range(out_ref.shape[0]):
                out_ref[k, pl.ds(4 * v + where_ref[b], 1)] = line
    for k in range(out_ref.shape[0]):
        out_ref[k, 20:24] = jnp.zeros((4, LANES), f32)


def total_of(lines):
    out = lines[0]
    for line in lines[1:]:
        out = out + line
    return out


def lse_of(lines):
    high = functools.reduce(jnp.maximum, lines)
    return high + jnp.log(total_of([jnp.exp(line - high) for line in lines]))


def merge_kernel(in_ref, out_ref):
    sources = in_ref.shape[0]
    for c in range(2):
        lines = [in_ref[s] for s in range(c, sources, 2)]
        lse, added = lse_of(lines), total_of(lines)
        for v in range(5):
            part = slice(4 * v, 4 * v + 4)
            value = (lse, added, lse, added, lines[0])[v]
            for k in range(out_ref.shape[0]):
                out_ref[k, v, 4 * c : 4 * c + 4] = value[part]


def as_row(column):
    n = column.shape[0]
    return jnp.sum(jnp.where(iota((n, n), 0) == iota((n, n), 1), column, 0), axis=0, keepdims=True)


def tables_kernel(me_ref, len_ref, owner_ref, score_ref, out_ref):
    me = me_ref[0]
    length, owner = len_ref[...], owner_ref[...]
    n = length.shape[1]
    sub, lane = iota((n, n), 0), iota((n, n), 1)
    length_col, owner_col = as_column(length), as_column(owner)
    earlier = lane < sub
    start = jnp.sum(jnp.where(earlier, length, 0), axis=1, keepdims=True)
    before = earlier & (owner_col == owner)
    offset = jnp.sum(jnp.where(before, length, 0), axis=1, keepdims=True)
    rank = jnp.sum(jnp.where(before, 1, 0), axis=1, keepdims=True)
    inside = (owner_col == me) & (lane >= offset) & (lane < offset + length_col)
    slot = jnp.sum(jnp.where(inside, start + lane - offset + 1, 0), axis=0, keepdims=True)
    slot = jnp.where(slot > 0, slot, -7)
    mine = owner_col == me
    table = jnp.zeros((n, n), f32)
    for k, value in enumerate(
        (
            start + 1,
            start + length_col + 1,
            as_column(slot),
            jnp.where(mine & (rank == 0), 1, 0),
            jnp.where(mine & (rank == 1), 1, 0),
        )
    ):
        table = jnp.where(lane == k, value.astype(f32), table)
    out_ref[...] = jnp.where(lane == 5, as_column(score_ref[...]), table)


def docs_kernel(in_ref, table_ref, token_ref, doc_ref):
    sources = in_ref.shape[0]
    table = table_ref[...]
    n = table.shape[0]
    low, high, slot, first, second, score = (table[:, k : k + 1] for k in range(6))
    count = jnp.zeros((n, LANES), f32)
    kl_sum, logprob = count, count
    for xl in range(2):
        lines = [[in_ref[s, v] for s in range(xl, sources, 2)] for v in range(5)]
        policy = total_of(lines[1]) - lse_of(lines[0])
        ratio = policy - (total_of(lines[3]) - lse_of(lines[2]))
        kl = 0.5 * ratio * ratio
        place = lines[4][0]
        for r in range(8):
            at = place[r : r + 1]
            within = (at >= low) & (at < high)
            count = count + jnp.where(within, 1.0, 0.0)
            kl_sum = kl_sum + jnp.where(within, kl[r : r + 1], 0.0)
            logprob = logprob + jnp.where(at == slot, policy[r : r + 1], 0.0)
    count = jnp.sum(count, axis=1, keepdims=True)
    kl_sum = jnp.sum(kl_sum, axis=1, keepdims=True)
    token_ref[...] = as_row(jnp.sum(logprob, axis=1, keepdims=True))
    reward = score - kl_weight * kl_sum / jnp.maximum(count, 1.0)
    baseline = jnp.sum(count * reward, axis=0, keepdims=True) / jnp.sum(
        count, axis=0, keepdims=True
    )
    advantage = reward - baseline
    doc_ref[:, 0:1] = jnp.sum(first * advantage, axis=0, keepdims=True)
    doc_ref[:, 1:2] = jnp.sum(second * advantage, axis=0, keepdims=True)


RESULT = pltpu.VMEM


def shape_of(shape, dtype):
    return jax.ShapeDtypeStruct(shape, dtype)


def shifted(x, axis, by):
    n = lax.axis_size(axis)
    return lax.ppermute(x, axis, [(i, (i + by) % n) for i in range(n)])


def one_device(
    hidden_policy,
    hidden_reference,
    gain_policy,
    gain_reference,
    head_policy,
    head_reference,
    targets,
    loss_mask,
    doc_lengths,
    doc_owner,
    doc_score,
):
    ny, nz, nx = lax.axis_size("y"), lax.axis_size("z"), lax.axis_size(X)
    tok, width = hidden_policy.shape
    columns = head_policy.shape[1]
    per, half = width // LANES, tok // 4
    me, x = lax.axis_index(ROWS), lax.axis_index(X)
    c = lax.axis_index("c")

    pair_policy = [(i, i ^ 1) for i in range(nx)]
    pair_reference = [(i, (i + 1) % nx if i % 2 else (i - 1) % nx) for i in range(nx)]
    near_policy = lax.ppermute(head_policy, X, pair_policy)
    near_reference = lax.ppermute(head_reference, X, pair_reference)
    swapped = [shifted(near_policy, "c", 1), shifted(near_reference, "c", 1)]
    other = [shifted(head_policy, "c", 1), shifted(head_reference, "c", 1)]
    heads = [
        head_policy,
        other[0],
        near_policy,
        swapped[0],
        head_reference,
        other[1],
        near_reference,
        swapped[1],
    ]
    x_policy = x ^ 1
    x_reference = jnp.where(x % 2 == 1, (x + 1) % nx, (x + nx - 1) % nx)
    row_of = me - c
    bases = jnp.stack(
        [
            ((row_of + core) * nx + place) * columns
            for partner in (x_policy, x_reference)
            for place in (x, partner)
            for core in (c, 1 - c)
        ]
    ).astype(jnp.int32)

    lines = 2 * per * half + 8
    sent = pl.pallas_call(
        pick_kernel,
        out_shape=shape_of((nz, nx, lines, LANES), bf16),
        in_specs=[VMEM] * 4,
        out_specs=VMEM,
        name="pick",
    )(hidden_policy, hidden_reference, targets[None, :], loss_mask[None, :])
    got = lax.all_to_all(
        sent.reshape(nz * nx, lines, LANES), ("z", *X), 0, 0, tiled=True
    ).reshape(nz, nx, lines, LANES)
    wide = 2 * nx * per * half + 8
    own = pl.pallas_call(
        norm_kernel,
        out_shape=[shape_of((nz // 2, wide, LANES), bf16)] * 2,
        in_specs=[VMEM] * 3,
        out_specs=[VMEM] * 2,
        name="norm",
    )(got, gain_policy[None, :], gain_reference[None, :])
    below_first, above_first = shifted(own[0], "y", 1), shifted(own[1], "y", -1)
    below_second, above_second = shifted(own[1], "y", 1), shifted(own[0], "y", -1)
    below, above = (below_first, below_second), (above_second, above_first)
    far = [shifted(below[0], "y", 1), shifted(above[1], "y", -1)]
    lengths, _ = lax.optimization_barrier((doc_lengths, (below_first, above_first)))
    table = pl.pallas_call(
        tables_kernel,
        out_shape=shape_of((LANES, LANES), f32),
        in_specs=[SMEM] + [VMEM] * 3,
        out_specs=VMEM,
        name="tables",
    )(
        jnp.stack([me]).astype(jnp.int32),
        lengths[None, :],
        doc_owner[None, :],
        doc_score[None, :],
    )
    y = lax.axis_index("y")
    order = [y, (y + ny - 1) % ny, (y + 1) % ny, (y + 2) % ny]
    where = jnp.stack(order + [(row * nz * 2 + c) * tok for row in order]).astype(jnp.int32)
    group = 2 * nz

    params = pltpu.CompilerParams(vmem_limit_bytes=24 * 1024 * 1024)
    depth, chunk = nx * width, own[0].shape
    cost = functools.partial(pl.CostEstimate, bytes_accessed=1 << 24, transcendentals=0)

    def local(tokens):
        blocks = len(tokens) // 2
        total = blocks * nz * half
        return pl.pallas_call(
            functools.partial(local_kernel, blocks),
            out_shape=(shape_of((blocks, 8, LANES), f32), shape_of((2, total, depth), bf16)),
            in_specs=[SMEM] + [ANY] * (len(tokens) + 4),
            out_specs=(VMEM, VMEM),
            scratch_shapes=[
                pltpu.VMEM((len(tokens), *chunk), bf16),
                pltpu.VMEM((total, columns), f32),
                pltpu.VMEM((total, columns), f32),
                pltpu.VMEM((8, depth, columns), bf16),
                pltpu.SemaphoreType.DMA((len(tokens),)),
                pltpu.SemaphoreType.DMA((4,)),
            ],
            compiler_params=params,
            cost_estimate=cost(flops=8 * total * depth * columns),
        )(bases, *tokens, heads[0], heads[1], heads[4], heads[5])

    mine, mine_lhs = local(own)
    beside, beside_lhs = local((*below, *above))
    total = ny * nz * half
    stats = pl.pallas_call(
        far_kernel,
        out_shape=RESULT((group, 24, LANES), f32),
        in_specs=[SMEM] * 2 + [ANY] * 16 + [VMEM] * 2 + [ANY] * 2,
        out_specs=VMEM,
        scratch_shapes=[
            pltpu.VMEM((2, *chunk), bf16),
            pltpu.VMEM((8, chunk[0], 8, LANES), bf16),
            pltpu.VMEM((2, total, depth), bf16),
            pltpu.VMEM((total - LANES, columns), f32),
            pltpu.VMEM((total - LANES, columns), f32),
            pltpu.VMEM((8, depth, columns), bf16),
            pltpu.SemaphoreType.DMA((2,)),
            pltpu.SemaphoreType.DMA((8,)),
            pltpu.SemaphoreType.DMA((2,)),
            pltpu.SemaphoreType.DMA((8,)),
        ],
        compiler_params=params,
        cost_estimate=cost(flops=10 * total * depth * columns),
        name="logits_far",
    )(bases, where, *own, *below, *above, *far, *heads, mine, beside, mine_lhs, beside_lhs)
    gathered = lax.all_to_all(stats, ("z", "c"), 0, 0, tiled=True)
    group = ny * nx
    merged = pl.pallas_call(
        merge_kernel,
        out_shape=RESULT((group, 5, 8, LANES), f32),
        in_specs=[VMEM],
        out_specs=VMEM,
        name="merge",
    )(gathered)
    everything = lax.all_to_all(merged, ("y", *X), 0, 0, tiled=True)
    token_logprob, advantage = pl.pallas_call(
        docs_kernel,
        out_shape=(shape_of((1, CAP), f32), shape_of((1, DOC_DEV), f32)),
        in_specs=[VMEM] * 2,
        out_specs=(VMEM, VMEM),
        name="docs",
    )(everything, table)
    return token_logprob.reshape(CAP), advantage.reshape(DOC_DEV)


def solution(mesh):
    finer = Mesh(
        mesh.devices.reshape(4, 8, 2, 2, mesh.shape["vocab"] // 2), ("y", "z", "c", "xh", "xl")
    )
    placed = (
        P(ROWS, X),
        P(ROWS, X),
        P(),
        P(),
        P(None, ALL),
        P(None, ALL),
        P(ROWS),
        P(ROWS),
        P(),
        P(),
        P(),
    )
    return jax.shard_map(
        one_device, mesh=finer, in_specs=placed, out_specs=(P(ROWS), P(ROWS)), check_vma=False
    )
```

```python
import functools

import jax
import jax.numpy as jnp
from jax import lax
from jax.experimental import pallas as pl
from jax.experimental.pallas import tpu as pltpu
from jax.sharding import Mesh
from jax.sharding import PartitionSpec as P


DOC_DEV = 2
CAP = 128
LANES = 128
ROWS = ("y", "z", "c")
X = ("xh", "xl")
ALL = ("y", "z", "c", "xh", "xl")

epsilon = 1e-06
kl_weight = 0.1
f32 = jnp.float32
bf16 = jnp.bfloat16
VMEM = pl.BlockSpec(memory_space=pltpu.VMEM)
SMEM = pl.BlockSpec(memory_space=pltpu.SMEM)
ANY = pl.BlockSpec(memory_space=pl.ANY)


def iota(shape, dim):
    return lax.broadcasted_iota(jnp.int32, shape, dim)


def as_column(row):
    n = row.shape[1]
    return jnp.sum(jnp.where(iota((n, n), 0) == iota((n, n), 1), row, 0), axis=1, keepdims=True)


def pick_kernel(hp_ref, hr_ref, tgt_ref, mask_ref, out_ref):
    tok = hp_ref.shape[0]
    kept, half = tok // 2, tok // 4
    nz, nx, lines, _ = out_ref.shape
    per = (lines - 8) // half // 2
    mask_row = mask_ref[...]
    mask_col = as_column(mask_row)
    sub, lane = iota((tok, tok), 0), iota((tok, tok), 1)
    rank = jnp.sum(jnp.where(sub <= lane, mask_col, 0), axis=0, keepdims=True) - 1
    select = (iota((kept, tok), 0) == rank) & (mask_row == 1)
    one_hot = select.astype(f32).astype(bf16)
    target = jnp.sum(jnp.where(select, tgt_ref[...], 0), axis=1, keepdims=True)
    place = jnp.sum(
        jnp.where(select, iota((kept, tok), 1) + 1, 0), axis=1, keepdims=True
    )
    packed = [
        jnp.dot(one_hot, ref[...], preferred_element_type=f32).astype(bf16)
        for ref in (hp_ref, hr_ref)
    ]
    spot = iota((8, LANES), 1)
    for h in range(2):
        digits = jnp.zeros((8, LANES), jnp.int32)
        for g in range(2):
            part = slice(h * half + g * 8, h * half + g * 8 + 8)
            for k, value in enumerate(
                (target[part] & 63, (target[part] >> 6) & 63, target[part] >> 12, place[part])
            ):
                digits = jnp.where(spot == 4 * g + k, value, digits)
        digits = digits.astype(f32).astype(bf16)
        rows = slice(h * half, (h + 1) * half)
        pieces = [
            packed[m][rows, j * LANES : (j + 1) * LANES] for m in range(2) for j in range(per)
        ]
        for z in range(nz):
            for x in range(h, nx, 2):
                for t, piece in enumerate(pieces):
                    out_ref[z, x, t * half : (t + 1) * half] = piece
                out_ref[z, x, 2 * per * half :] = digits


def norm_kernel(in_ref, gp_ref, gr_ref, *out_refs):
    nz, nx, lines, _ = in_ref.shape
    half = 16
    per = (lines - 8) // half // 2
    width = nx * per * LANES
    share = nz // len(out_refs)
    for z in range(nz):
        out_ref, at = out_refs[z // share], z % share
        for m, gain_ref in enumerate((gp_ref, gr_ref)):
            parts = [
                in_ref[z, x, (m * per + j) * half : (m * per + j + 1) * half].astype(f32)
                for x in range(nx)
                for j in range(per)
            ]
            square = parts[0] * parts[0]
            for part in parts[1:]:
                square = square + part * part
            mean = jnp.sum(square, axis=1, keepdims=True) * (1.0 / width)
            inverse = lax.rsqrt(mean + epsilon)
            for k, part in enumerate(parts):
                gain = gain_ref[:, k * LANES : (k + 1) * LANES].astype(f32)
                t = m * nx * per + k
                out_ref[at, t * half : (t + 1) * half] = (part * inverse * gain).astype(bf16)
        out_ref[at, 2 * nx * per * half :] = in_ref[z, 0, 2 * per * half :]


def place_lines(tok, lhs, line):
    half = 16
    share, lines, _ = tok.shape
    per = (lines - 8) // half // 2
    for at in range(share):
        for m in range(2):
            for k in range(per):
                t = m * per + k
                lhs[m, line : line + half, k * LANES : (k + 1) * LANES] = tok[
                    at, t * half : (t + 1) * half
                ]
        line += half


def columns_of(digit_refs):
    target, place = [], []
    for ref in digit_refs:
        for at in range(ref.shape[0]):
            digit = ref[at].astype(f32)
            for g in (0, 4):
                target.append(
                    digit[:, g : g + 1]
                    + 64.0 * digit[:, g + 1 : g + 2]
                    + 4096.0 * digit[:, g + 2 : g + 3]
                )
                place.append(digit[:, g + 3 : g + 4])
    return jnp.concatenate(target, axis=0).astype(jnp.int32), jnp.concatenate(place, axis=0)


def scores(lhs, rows, target, shards, heads, base_ref, buffers, waits):
    total, columns = rows.stop - rows.start, heads.shape[2]
    column = iota((total, columns), 1)

    def product(i, out):
        if i in waits:
            waits.pop(i).wait()
        out[0:total] = jnp.dot(lhs[i // 4, rows], heads[i], preferred_element_type=f32)

    def reduce(i, out, state):
        values = out[0:total]
        new_high = jnp.max(values, axis=1, keepdims=True)
        match = column == target - base_ref[i]
        new_hit = jnp.sum(jnp.where(match, values, 0.0), axis=1, keepdims=True)
        if state is None:
            part = jnp.sum(jnp.exp(values - new_high), axis=1, keepdims=True)
            return new_high, part, new_hit
        high, summed, hit = state
        new_high = jnp.maximum(high, new_high)
        part = jnp.sum(jnp.exp(values - new_high), axis=1, keepdims=True)
        return new_high, summed * jnp.exp(high - new_high) + part, hit + new_hit

    found = [None, None]
    product(shards[0], buffers[0])
    for n, i in enumerate(shards):
        if n + 1 < len(shards):
            product(shards[n + 1], buffers[(n + 1) % 2])
        found[i // 4] = reduce(i, buffers[n % 2], found[i // 4])
    return [
        value for high, summed, hit in found for value in (high + jnp.log(summed), hit)
    ]


def as_line(column):
    diagonal = iota((LANES, LANES), 0) == iota((LANES, LANES), 1)
    return jnp.sum(jnp.where(diagonal, column, 0.0), axis=0, keepdims=True)


def bring(sources, into, sem):
    copies = [pltpu.make_async_copy(ref, into.at[k], sem.at[k]) for k, ref in enumerate(sources)]
    for copy in copies:
        copy.start()
    return copies


def local_kernel(blocks, base_ref, *refs):
    sources, head_sources = refs[: 2 * blocks], refs[2 * blocks : 2 * blocks + 4]
    out_ref, lhs, toks, even, odd, heads, tok_sem, sem = refs[2 * blocks + 4 :]
    shards = (0, 1, 4, 5)
    arriving = bring(sources, toks, tok_sem)
    waits = {
        i: pltpu.make_async_copy(source, heads.at[i], sem.at[n])
        for n, (i, source) in enumerate(zip(shards, head_sources))
    }
    for copy in waits.values():
        copy.start()
    for k, copy in enumerate(arriving):
        copy.wait()
        place_lines(toks.at[k], lhs, k * LANES // 2)
    last = toks.shape[2] - 8
    target, _ = columns_of([toks.at[k, :, last:] for k in range(2 * blocks)])
    rows = slice(0, blocks * LANES)
    values = scores(lhs, rows, target, shards, heads, base_ref, (even, odd), waits)
    for b in range(blocks):
        for v, value in enumerate(values):
            out_ref[b, v : v + 1] = as_line(value[b * LANES : (b + 1) * LANES])
        out_ref[b, 4:8] = jnp.zeros((4, LANES), f32)


def far_kernel(base_ref, *refs):
    sources, head_sources, done, packed = refs[:8], refs[8:16], refs[16:18], refs[18:20]
    out_ref, toks, digits, lhs, even, odd, heads, tok_sem, digit_sem, pack_sem, sem = refs[20:]
    lines = sources[0].shape[1]
    arriving = bring(sources[6:], toks, tok_sem)
    arriving += bring([ref.at[:, lines - 8 :] for ref in sources], digits, digit_sem)
    for k, (start, stop) in enumerate(((0, LANES), (LANES, 3 * LANES))):
        copy = pltpu.make_async_copy(packed[k], lhs.at[:, start:stop], pack_sem.at[k])
        copy.start()
        arriving.append(copy)
    order = (2, 3, 6, 7, 0, 1, 4, 5)
    waits = {i: pltpu.make_async_copy(head_sources[i], heads.at[i], sem.at[i]) for i in order}
    for copy in waits.values():
        copy.start()
    for copy in arriving:
        copy.wait()
    near = 3 * LANES
    place_lines(toks.at[0], lhs, near)
    place_lines(toks.at[1], lhs, near + LANES // 2)
    target, place = columns_of([digits.at[k] for k in range(8)])
    first = scores(
        lhs, slice(0, near), target[:near], (2, 3, 6, 7), heads, base_ref, (even, odd), waits
    )
    last = scores(
        lhs,
        slice(near, near + LANES),
        target[near:],
        (2, 3, 0, 1, 6, 7, 4, 5),
        heads,
        base_ref,
        (even, odd),
        waits,
    )
    index_z = iota((1, LANES), 1) // 16
    for b in range(4):
        at = slice(b * LANES, (b + 1) * LANES)
        for v in range(5):
            if v == 4:
                line = as_line(place[at])
                line = jnp.where(
                    line > 0.0, line + (base_ref[12 + b] + 128 * index_z).astype(f32), 0.0
                )
            elif b == 3:
                line = as_line(last[v])
            else:
                local = done[0][0, v : v + 1] if b == 0 else done[1][b - 1, v : v + 1]
                line = as_line(first[v][at])
                line = lse_of([line, local]) if v % 2 == 0 else line + local
            for k in range(out_ref.shape[0]):
                out_ref[k, pl.ds(4 * v + base_ref[8 + b], 1)] = line
    for k in range(out_ref.shape[0]):
        out_ref[k, 20:24] = jnp.zeros((4, LANES), f32)


def total_of(lines):
    out = lines[0]
    for line in lines[1:]:
        out = out + line
    return out


def lse_of(lines):
    high = functools.reduce(jnp.maximum, lines)
    return high + jnp.log(total_of([jnp.exp(line - high) for line in lines]))


def merge_kernel(in_ref, out_ref):
    sources = in_ref.shape[0]
    for c in range(2):
        lines = [in_ref[s] for s in range(c, sources, 2)]
        lse, added = lse_of(lines), total_of(lines)
        for v in range(5):
            part = slice(4 * v, 4 * v + 4)
            value = (lse, added, lse, added, lines[0])[v]
            for k in range(out_ref.shape[0]):
                out_ref[k, v, 4 * c : 4 * c + 4] = value[part]


def as_row(column):
    n = column.shape[0]
    return jnp.sum(jnp.where(iota((n, n), 0) == iota((n, n), 1), column, 0), axis=0, keepdims=True)


def tables_kernel(me_ref, len_ref, owner_ref, score_ref, out_ref):
    me = me_ref[0]
    length, owner = len_ref[...], owner_ref[...]
    n = length.shape[1]
    sub, lane = iota((n, n), 0), iota((n, n), 1)
    length_col, owner_col = as_column(length), as_column(owner)
    earlier = lane < sub
    start = jnp.sum(jnp.where(earlier, length, 0), axis=1, keepdims=True)
    before = earlier & (owner_col == owner)
    offset = jnp.sum(jnp.where(before, length, 0), axis=1, keepdims=True)
    rank = jnp.sum(jnp.where(before, 1, 0), axis=1, keepdims=True)
    inside = (owner_col == me) & (lane >= offset) & (lane < offset + length_col)
    slot = jnp.sum(jnp.where(inside, start + lane - offset + 1, 0), axis=0, keepdims=True)
    slot = jnp.where(slot > 0, slot, -7)
    mine = owner_col == me
    table = jnp.zeros((n, n), f32)
    for k, value in enumerate(
        (
            start + 1,
            start + length_col + 1,
            as_column(slot),
            jnp.where(mine & (rank == 0), 1, 0),
            jnp.where(mine & (rank == 1), 1, 0),
        )
    ):
        table = jnp.where(lane == k, value.astype(f32), table)
    out_ref[...] = jnp.where(lane == 5, as_column(score_ref[...]), table)


def docs_kernel(in_ref, table_ref, token_ref, doc_ref):
    sources = in_ref.shape[0]
    table = table_ref[...]
    n = table.shape[0]
    low, high, slot, first, second, score = (table[:, k : k + 1] for k in range(6))
    count = jnp.zeros((n, LANES), f32)
    kl_sum, logprob = count, count
    for xl in range(2):
        lines = [[in_ref[s, v] for s in range(xl, sources, 2)] for v in range(5)]
        policy = total_of(lines[1]) - lse_of(lines[0])
        ratio = policy - (total_of(lines[3]) - lse_of(lines[2]))
        kl = 0.5 * ratio * ratio
        place = lines[4][0]
        for r in range(8):
            at = place[r : r + 1]
            within = (at >= low) & (at < high)
            count = count + jnp.where(within, 1.0, 0.0)
            kl_sum = kl_sum + jnp.where(within, kl[r : r + 1], 0.0)
            logprob = logprob + jnp.where(at == slot, policy[r : r + 1], 0.0)
    count = jnp.sum(count, axis=1, keepdims=True)
    kl_sum = jnp.sum(kl_sum, axis=1, keepdims=True)
    token_ref[...] = as_row(jnp.sum(logprob, axis=1, keepdims=True))
    reward = score - kl_weight * kl_sum / jnp.maximum(count, 1.0)
    baseline = jnp.sum(count * reward, axis=0, keepdims=True) / jnp.sum(
        count, axis=0, keepdims=True
    )
    advantage = reward - baseline
    doc_ref[:, 0:1] = jnp.sum(first * advantage, axis=0, keepdims=True)
    doc_ref[:, 1:2] = jnp.sum(second * advantage, axis=0, keepdims=True)


RESULT = pltpu.VMEM


def shape_of(shape, dtype):
    return jax.ShapeDtypeStruct(shape, dtype)


def shifted(x, axis, by):
    n = lax.axis_size(axis)
    return lax.ppermute(x, axis, [(i, (i + by) % n) for i in range(n)])


def one_device(
    hidden_policy,
    hidden_reference,
    gain_policy,
    gain_reference,
    head_policy,
    head_reference,
    targets,
    loss_mask,
    doc_lengths,
    doc_owner,
    doc_score,
):
    ny, nz, nx = lax.axis_size("y"), lax.axis_size("z"), lax.axis_size(X)
    tok, width = hidden_policy.shape
    columns = head_policy.shape[1]
    per, half = width // LANES, tok // 4
    me, x = lax.axis_index(ROWS), lax.axis_index(X)
    c = lax.axis_index("c")

    pair_policy = [(i, i ^ 1) for i in range(nx)]
    pair_reference = [(i, (i + 1) % nx if i % 2 else (i - 1) % nx) for i in range(nx)]
    near_policy = lax.ppermute(head_policy, X, pair_policy)
    near_reference = lax.ppermute(head_reference, X, pair_reference)
    swapped = [shifted(near_policy, "c", 1), shifted(near_reference, "c", 1)]
    other = [shifted(head_policy, "c", 1), shifted(head_reference, "c", 1)]
    heads = [
        head_policy,
        other[0],
        near_policy,
        swapped[0],
        head_reference,
        other[1],
        near_reference,
        swapped[1],
    ]
    x_policy = x ^ 1
    x_reference = jnp.where(x % 2 == 1, (x + 1) % nx, (x + nx - 1) % nx)
    row_of = me - c
    y = lax.axis_index("y")
    order = [y, (y + ny - 1) % ny, (y + 1) % ny, (y + 2) % ny]
    bases = jnp.stack(
        [
            ((row_of + core) * nx + place) * columns
            for partner in (x_policy, x_reference)
            for place in (x, partner)
            for core in (c, 1 - c)
        ]
        + order
        + [(row * nz * 2 + c) * tok for row in order]
    ).astype(jnp.int32)

    lines = 2 * per * half + 8
    sent = pl.pallas_call(
        pick_kernel,
        out_shape=shape_of((nz, nx, lines, LANES), bf16),
        in_specs=[VMEM] * 4,
        out_specs=VMEM,
        name="pick",
    )(hidden_policy, hidden_reference, targets[None, :], loss_mask[None, :])
    got = lax.all_to_all(
        sent.reshape(nz * nx, lines, LANES), ("z", *X), 0, 0, tiled=True
    ).reshape(nz, nx, lines, LANES)
    wide = 2 * nx * per * half + 8
    own = pl.pallas_call(
        norm_kernel,
        out_shape=[shape_of((nz // 2, wide, LANES), bf16)] * 2,
        in_specs=[VMEM] * 3,
        out_specs=[VMEM] * 2,
        name="norm",
    )(got, gain_policy[None, :], gain_reference[None, :])
    below_first, above_first = shifted(own[0], "y", 1), shifted(own[1], "y", -1)
    below_second, above_second = shifted(own[1], "y", 1), shifted(own[0], "y", -1)
    below, above = (below_first, below_second), (above_second, above_first)
    far = [shifted(below[0], "y", 1), shifted(above[1], "y", -1)]
    lengths, _ = lax.optimization_barrier((doc_lengths, (below_first, above_first)))
    table = pl.pallas_call(
        tables_kernel,
        out_shape=shape_of((LANES, LANES), f32),
        in_specs=[SMEM] + [VMEM] * 3,
        out_specs=VMEM,
        name="tables",
    )(
        jnp.stack([me]).astype(jnp.int32),
        lengths[None, :],
        doc_owner[None, :],
        doc_score[None, :],
    )
    group = 2 * nz

    params = pltpu.CompilerParams(vmem_limit_bytes=24 * 1024 * 1024)
    depth, chunk = nx * width, own[0].shape
    cost = functools.partial(pl.CostEstimate, bytes_accessed=1 << 24, transcendentals=0)

    def local(tokens):
        blocks = len(tokens) // 2
        total = blocks * nz * half
        return pl.pallas_call(
            functools.partial(local_kernel, blocks),
            out_shape=(shape_of((blocks, 8, LANES), f32), shape_of((2, total, depth), bf16)),
            in_specs=[SMEM] + [ANY] * (len(tokens) + 4),
            out_specs=(VMEM, VMEM),
            scratch_shapes=[
                pltpu.VMEM((len(tokens), *chunk), bf16),
                pltpu.VMEM((total, columns), f32),
                pltpu.VMEM((total, columns), f32),
                pltpu.VMEM((8, depth, columns), bf16),
                pltpu.SemaphoreType.DMA((len(tokens),)),
                pltpu.SemaphoreType.DMA((4,)),
            ],
            compiler_params=params,
            cost_estimate=cost(flops=8 * total * depth * columns),
        )(bases, *tokens, heads[0], heads[1], heads[4], heads[5])

    mine, mine_lhs = local(own)
    beside, beside_lhs = local((*below, *above))
    total = ny * nz * half
    stats = pl.pallas_call(
        far_kernel,
        out_shape=RESULT((group, 24, LANES), f32),
        in_specs=[SMEM] + [ANY] * 16 + [VMEM] * 2 + [ANY] * 2,
        out_specs=VMEM,
        scratch_shapes=[
            pltpu.VMEM((2, *chunk), bf16),
            pltpu.VMEM((8, chunk[0], 8, LANES), bf16),
            pltpu.VMEM((2, total, depth), bf16),
            pltpu.VMEM((total - LANES, columns), f32),
            pltpu.VMEM((total - LANES, columns), f32),
            pltpu.VMEM((8, depth, columns), bf16),
            pltpu.SemaphoreType.DMA((2,)),
            pltpu.SemaphoreType.DMA((8,)),
            pltpu.SemaphoreType.DMA((2,)),
            pltpu.SemaphoreType.DMA((8,)),
        ],
        compiler_params=params,
        cost_estimate=cost(flops=10 * total * depth * columns),
        name="logits_far",
    )(bases, *own, *below, *above, *far, *heads, mine, beside, mine_lhs, beside_lhs)
    gathered = lax.all_to_all(stats, ("z", "c"), 0, 0, tiled=True)
    group = ny * nx
    merged = pl.pallas_call(
        merge_kernel,
        out_shape=RESULT((group, 5, 8, LANES), f32),
        in_specs=[VMEM],
        out_specs=VMEM,
        name="merge",
    )(gathered)
    everything = lax.all_to_all(merged, ("y", *X), 0, 0, tiled=True)
    token_logprob, advantage = pl.pallas_call(
        docs_kernel,
        out_shape=(shape_of((1, CAP), f32), shape_of((1, DOC_DEV), f32)),
        in_specs=[VMEM] * 2,
        out_specs=(VMEM, VMEM),
        name="docs",
    )(everything, table)
    return token_logprob.reshape(CAP), advantage.reshape(DOC_DEV)


def solution(mesh):
    finer = Mesh(
        mesh.devices.reshape(4, 8, 2, 2, mesh.shape["vocab"] // 2), ("y", "z", "c", "xh", "xl")
    )
    placed = (
        P(ROWS, X),
        P(ROWS, X),
        P(),
        P(),
        P(None, ALL),
        P(None, ALL),
        P(ROWS),
        P(ROWS),
        P(),
        P(),
        P(),
    )
    return jax.shard_map(
        one_device, mesh=finer, in_specs=placed, out_specs=(P(ROWS), P(ROWS)), check_vma=False
    )
```
